512 devices in a mesh: term: 64 (over z, x), sector: 8 (over y, core).
Axes of the slice: x: 4, y: 4, z: 16, core: 2. Of those that a mesh axis runs over, the one named last changes fastest.
Arguments:
- wave_blocks: bfloat16 [16, 512, 512], P(None, 'term'), may hold values from -0.59765625 to 0.59765625
- left_ops: bfloat16 [8, 128, 512, 512], P('sector', 'term'), may hold values from -0.25 to 0.25
- right_ops: bfloat16 [8, 256, 512, 512], P('sector', 'term'), may hold values from -0.25 to 0.25
- wanted: int32 [8, 64, 2], P('sector'), may hold values from 0 to 15, as said below
- pairs: int32 [8, 64, 12], P('sector', 'term'), may hold values from 0 to 15, as said below
- targets: int32 [8, 64, 12], P('sector', 'term'), may hold values from 0 to 1
- live: int32 [8, 64], P('sector', 'term'), may hold values from 1 to 12, as said below
Outputs:
- sigma: float32 [16, 512, 512], P('sector', 'term')
The draws below stay inside these ranges and needn't reach their ends.
Inputs may be any that keep to these rules, and one draw needn't show every extreme that they name: `wanted`: the sectors listed for one section are distinct. `pairs`: codes are distinct within a section; a code c names half product c // 4 and right operator c % 4 of the section. Only the first live slots of a section are used; in every draw some section has 12 live slots.
All inputs are finite; a program needn't handle non-finite values.
Results may differ from the reference program's by a relative error of at most 0.0029.
Values may be sent and summed in bfloat16 or wider, within the bound.
A program may use at most 64 MiB of HBM per device.

```python
import jax
import jax.numpy as jnp
from jax import lax

B = 512
SEC_DEV = 2
NEED_DEV = 2
OPS_L = 2
OPS_R = 4
TERM_DEV = 12
GROUPS = 8
SECTIONS = 64
SECTORS = 16
HALVES = 4


def pick_distinct(key, pool, taken):
    keys = jax.random.split(key, GROUPS * SECTIONS)

    def one_pick(one_key):
        return jax.random.permutation(one_key, pool)[:taken]
    picks = jax.vmap(one_pick)(keys)
    return picks.reshape(GROUPS, SECTIONS, taken).astype(jnp.int32)


def draw_wanted(key, part):
    return pick_distinct(jax.random.fold_in(key, 11), SECTORS, NEED_DEV)


def draw_pairs(key, part):
    return pick_distinct(jax.random.fold_in(key, 23), HALVES * OPS_R, TERM_DEV)


def draw_live(key, part):
    first_key = jax.random.fold_in(key, 37)
    second_key = jax.random.fold_in(key, 41)
    counts = jax.random.randint(first_key, (GROUPS * SECTIONS,), 1, TERM_DEV + 1)
    fullest = jax.random.randint(second_key, (), 0, GROUPS * SECTIONS)
    counts = counts.at[fullest].set(TERM_DEV)
    return counts.reshape(GROUPS, SECTIONS).astype(jnp.int32)


def plant(drawn, key, smallest, top_value):
    dims = drawn.shape
    spot = [jax.random.randint(jax.random.fold_in(key, axis), (), 0, dims[axis]) for axis in range(len(dims))]
    drawn = drawn.at[tuple(spot)].set(smallest)
    longest = dims.index(max(dims))
    spot[longest] = (spot[longest] + 1) % dims[longest]
    return drawn.at[tuple(spot)].set(top_value)


def levels(own_key, dims, cuts, least, largest):
    def one(position, shards_of):
        draws = jax.random.uniform(jax.random.fold_in(jax.random.fold_in(own_key, 6), position), (shards_of,), jnp.float32, least / len(cuts), largest / len(cuts))
        return jnp.repeat(jnp.exp(draws), dims[position] // shards_of).reshape((-1,) + (1,) * (len(dims) - position - 1))

    level = one(*cuts[0])
    for cut in cuts[1:]:
        level = level * one(*cut)
    return level


def noise(key, shape, deviation, most, shards=(), kind=jnp.bfloat16):
    loudness = levels(key, shape, shards, -0.22, 0.18) if shards else 1.0
    result = jax.random.normal(key, shape, jnp.float32) * deviation * loudness
    return jnp.minimum(jnp.maximum(result, -most), most).astype(kind)


def setup_inputs(seed: int = 0) -> dict:
    seeds = jax.random.split(jax.random.key(seed), 8)
    return {
        "wave_blocks": noise(seeds[0], (SECTORS, B, B), 0.1, 0.59765625, ((1, 64),)),
        "left_ops": noise(seeds[1], (GROUPS, SECTIONS * OPS_L, B, B), B ** -0.5, 0.25, ((0, 8), (1, 64))),
        "right_ops": noise(seeds[2], (GROUPS, SECTIONS * OPS_R, B, B), B ** -0.5, 0.25, ((0, 8), (1, 64))),
        "wanted": draw_wanted(jax.random.fold_in(seeds[7], 71), 0),
        "pairs": draw_pairs(jax.random.fold_in(seeds[7], 71), 0),
        "targets": plant(jax.random.randint(seeds[5], (GROUPS, SECTIONS, TERM_DEV), 0, SEC_DEV), jax.random.fold_in(seeds[5], 1), 0, SEC_DEV - 1).astype(jnp.int32),
        "live": draw_live(jax.random.fold_in(seeds[7], 71), 0),
    }


def reference(wave_blocks, left_ops, right_ops, wanted, pairs, targets, live):
    highest = lax.Precision.HIGHEST
    wave_wide = wave_blocks.astype(jnp.float32)
    sigma_start = jnp.zeros((SECTORS, B, B), jnp.float32)

    def device_step(sigma, device_flat):
        group_index = device_flat // SECTIONS
        section_index = device_flat % SECTIONS
        lefts = lax.dynamic_slice_in_dim(left_ops[group_index], section_index * OPS_L, OPS_L, 0).astype(jnp.float32)
        rights = lax.dynamic_slice_in_dim(right_ops[group_index], section_index * OPS_R, OPS_R, 0).astype(jnp.float32)
        sources = wanted[group_index, section_index].astype(jnp.int32)
        blocks = jnp.take(wave_wide, sources, axis=0)
        halves = jnp.einsum("aij,njk->anik", lefts, blocks, precision=highest)
        halves = lax.optimization_barrier(halves.astype(jnp.bfloat16)).astype(jnp.float32)
        halves = halves.reshape(HALVES, B, B)

        def slot_step(sigma_now, slot):
            pair_code = pairs[group_index, section_index, slot]
            product = jnp.dot(halves[pair_code // OPS_R], rights[pair_code % OPS_R].T, precision=highest)
            weight = (slot < live[group_index, section_index]).astype(jnp.float32)
            owner = (group_index * SEC_DEV + targets[group_index, section_index, slot]).astype(jnp.int32)
            current = lax.dynamic_index_in_dim(sigma_now, owner, 0, keepdims=False)
            sigma_now = lax.dynamic_update_index_in_dim(sigma_now, current + weight * product, owner, 0)
            return sigma_now, None

        sigma, unused = lax.scan(slot_step, sigma, jnp.arange(TERM_DEV, dtype=jnp.int32))
        return sigma, None

    sigma, unused = lax.scan(device_step, sigma_start, jnp.arange(GROUPS * SECTIONS, dtype=jnp.int32))
    return sigma
```

```python
import jax
import jax.numpy as jnp
from jax import lax
from jax.experimental import pallas as pl
from jax.experimental.pallas import tpu as pltpu
from jax.sharding import PartitionSpec as P

MESH = pl.DeviceIdType.MESH
NX, NY, NZ = 4, 4, 16
SLAB = NX * NY * 2
NZH = NZ // 2
OFFS = (2, 1, 3, 0)


def place():
    term = lax.axis_index("term")
    sector = lax.axis_index("sector")
    z, x = term // NX, lax.rem(term, NX)
    y, c = sector // 2, lax.rem(sector, 2)
    return z, x, y, c


def dev(z, x, y, c):
    return (z * NX + x, y * 2 + c)


def remote(src, dst, send, recv, target):
    return pltpu.make_async_remote_copy(
        src_ref=src, dst_ref=dst, send_sem=send, recv_sem=recv, device_id=target, device_id_type=MESH
    )


def wave_kernel(wave_ref, want_ref, w_ref, held, packed, want_v, want_s, send1, recv1, send2, recv2, sendw, recvw, local):
    z, x, y, c = place()
    sector = y * 2 + c
    barrier = pltpu.get_barrier_semaphore()

    def greet_z(d, _):
        pl.semaphore_signal(barrier, inc=1, device_id=dev(lax.rem(z + d, NZ), x, y, c), device_id_type=MESH)
        return 0

    def slab_core(e):
        return lax.rem(x + e // 8, NX), lax.rem(y + lax.rem(e, 8) // 2, NY), lax.rem(c + e, 2)

    def greet_slab(e, _):
        tx, ty, tc = slab_core(e)
        pl.semaphore_signal(barrier, inc=1, device_id=dev(z, tx, ty, tc), device_id_type=MESH)
        return 0

    lax.fori_loop(1, NZ, greet_z, 0)
    lax.fori_loop(1, SLAB, greet_slab, 0)
    pl.semaphore_wait(barrier, NZ - 1 + SLAB - 1)

    cols = pl.ds(pl.multiple_of(y * 128, 128), 128)
    zm = lax.rem(z, NZH)

    def stage1(i, there):
        tz = lax.rem(z + jnp.where(c == 0, i, NZ - i), NZ)
        fz = lax.rem(z + jnp.where(c == 0, NZ - i, i), NZ)
        slot = zm if there else lax.rem(fz, NZH)
        return remote(wave_ref.at[:, :, cols], held.at[slot], send1.at[i - 1], recv1.at[i - 1], dev(tz, x, y, c))

    def start1(i, _):
        stage1(i, True).start()
        return 0

    def wantcopy(e):
        ty, tc = lax.rem(y + e // 2, NY), lax.rem(c + e, 2)
        return remote(want_ref.at[z], want_v.at[sector], sendw.at[e], recvw.at[e], dev(z, x, ty, tc))

    for e in range(1, 8):
        wantcopy(e).start()
    lax.fori_loop(1, NZH, start1, 0)

    @pl.when(c == 0)
    def _():
        stage1(NZH, True).start()

    @pl.when(c == 1)
    def _():
        held[zm] = wave_ref[:, :, cols]

    want_v[sector] = want_ref[z]
    for e in range(1, 8):
        wantcopy(e).wait()
    copy = pltpu.make_async_copy(want_v, want_s, local)
    copy.start()
    copy.wait()

    def wait1(i, _):
        stage1(i, False).wait()
        return 0

    lax.fori_loop(1, NZH, wait1, 0)

    @pl.when(c == 0)
    def _():
        stage1(NZH, False).wait()

    def stage2(e):
        tx, ty, tc = slab_core(e)
        return remote(packed.at[e], w_ref.at[:, c, :, x, :, cols], send2.at[e], recv2.at[e], dev(z, tx, ty, tc))

    def pack(e, _):
        tx, ty, tc = slab_core(e)
        for j in range(2):
            source = want_s[ty * 2 + tc, 0, tx * 2 + j]
            packed[e, j] = held[:, source]
        stage2(e).start()
        return 0

    lax.fori_loop(1, SLAB, pack, 0)
    for j in range(2):
        source = want_s[sector, 0, x * 2 + j]
        w_ref[j, c, :, x, :, cols] = held[:, source]

    def wait2(e, _):
        stage2(e).wait()
        return 0

    lax.fori_loop(1, SLAB, wait2, 0)


def exchange_wave(wave, want):
    return pl.pallas_call(
        wave_kernel,
        out_shape=jax.ShapeDtypeStruct((2, 2, NZH, NX, 8, 512), jnp.bfloat16),
        in_specs=[pl.BlockSpec(memory_space=pltpu.VMEM)] * 2,
        out_specs=pl.BlockSpec(memory_space=pltpu.VMEM),
        scratch_shapes=[
            pltpu.VMEM((NZH, 16, 8, 128), jnp.bfloat16),
            pltpu.VMEM((SLAB, 2, NZH, 8, 128), jnp.bfloat16),
            pltpu.VMEM((8, 1, 128), jnp.int32),
            pltpu.SMEM((8, 1, 128), jnp.int32),
            pltpu.SemaphoreType.DMA((NZH,)),
            pltpu.SemaphoreType.DMA((NZH,)),
            pltpu.SemaphoreType.DMA((SLAB,)),
            pltpu.SemaphoreType.DMA((SLAB,)),
            pltpu.SemaphoreType.DMA((8,)),
            pltpu.SemaphoreType.DMA((8,)),
            pltpu.SemaphoreType.DMA,
        ],
        compiler_params=pltpu.CompilerParams(collective_id=0, has_side_effects=True),
    )(wave, want)


def sigma_kernel(
    w_ref, l_ref, r_ref, pairs, targets, live, out_ref, lp, halves, acc, xsend, xrecv, xown, zsend, zrecv, zown,
    sendx, recvx, sendz, recvz,
):
    z, x, y, c = place()
    barrier = pltpu.get_barrier_semaphore()

    def greet_z(d, _):
        pl.semaphore_signal(barrier, inc=1, device_id=dev(lax.rem(z + d, NZ), x, y, c), device_id_type=MESH)
        return 0

    lax.fori_loop(1, NZ, greet_z, 0)
    for e in range(1, NX):
        pl.semaphore_signal(barrier, inc=1, device_id=dev(z, lax.rem(x + e, NX), y, c), device_id_type=MESH)

    zb, zm = z // NZH, lax.rem(z, NZH)
    m = lax.broadcasted_iota(jnp.int32, (512, 256), 1) // (NX * 8)
    upper = (m >= zm) == (zb == 1)
    for a in range(2):
        low, high = l_ref[a, :, :256], l_ref[a, :, 256:]
        lp[a, :, 256:] = jnp.where(upper, high, low)
        lp[a, :, :256] = jnp.where(upper, low, high)

    def x_copy(q, e):
        return remote(
            xsend.at[q, e], xrecv.at[q, e], sendx.at[q, e], recvx.at[q, e], dev(z, lax.rem(x + e, NX), y, c)
        )

    def region(q):
        return lax.rem(z // 4 + OFFS[q], 4)

    def compute(q):
        rows = pl.ds(pl.multiple_of(region(q) * 128, 128), 128)
        for a in range(2):
            left = lp[a, rows, :]
            for j in range(2):
                half = jnp.dot(left, w_ref[j], preferred_element_type=jnp.float32)
                halves[a * 2 + j] = half.astype(jnp.bfloat16)
        acc[...] = jnp.zeros_like(acc)

        def slot_step(k, _):
            code = pairs[0, 0, k]
            product = lax.dot_general(
                halves[code // 4],
                r_ref[lax.rem(code, 4)],
                (((1,), (1,)), ((), ())),
                preferred_element_type=jnp.float32,
            )
            product = product.reshape(4, NX, 8, 512)
            used = k < live[0, 0]
            for t in range(2):
                acc[t] += jnp.where(used & (targets[0, 0, k] == t), product, 0.0)
            return 0

        lax.fori_loop(0, 12, slot_step, 0)
        for t in range(2):
            xown[q, t] = acc[t, :, x]
            for e in range(1, NX):
                xsend[q, e, t] = acc[t, :, lax.rem(x + e, NX)].astype(jnp.bfloat16)

    def z_copy(q, zz):
        tz = region(q) * 4 + zz
        return tz, lambda: remote(zsend.at[q, zz], zrecv.at[z], sendz.at[q, zz], recvz.at[z], dev(tz, x, y, c))

    def finish_x(q):
        for e in range(1, NX):
            x_copy(q, e).wait()
        for zz in range(4):
            tz, make = z_copy(q, zz)
            for t in range(2):
                total = xown[q, t, zz]
                for e in range(1, NX):
                    total = total + xrecv[q, e, t, zz].astype(jnp.float32)
                zsend[q, zz, t] = total.astype(jnp.bfloat16)
                if OFFS[q] == 0:

                    @pl.when(tz == z)
                    def _():
                        zown[t] = total

            if OFFS[q] == 0:

                @pl.when(tz != z)
                def _():
                    make().start()
            else:
                make().start()

    for q in range(4):
        compute(q)
        if q == 0:
            pl.semaphore_wait(barrier, NZ - 1 + NX - 1)
        for e in range(1, NX):
            x_copy(q, e).start()
        if q > 0:
            finish_x(q - 1)
    finish_x(3)

    for q in range(4):
        for zz in range(4):
            tz, make = z_copy(q, zz)
            if OFFS[q] == 0:

                @pl.when(tz != z)
                def _():
                    make().wait_send()
            else:
                make().wait_send()

    out_ref[...] = zown[...]

    def add(d, _):
        fz = lax.rem(z + d, NZ)
        remote(zsend.at[0, 0], zrecv.at[fz], sendz.at[0, 0], recvz.at[fz], dev(fz, x, y, c)).wait_recv()
        out_ref[...] += zrecv[fz].astype(jnp.float32)
        return 0

    lax.fori_loop(1, NZ, add, 0)


def sigma_rows(w, left, right, pairs, targets, live):
    vmem = pl.BlockSpec(memory_space=pltpu.VMEM)
    smem = pl.BlockSpec(memory_space=pltpu.SMEM)
    return pl.pallas_call(
        sigma_kernel,
        out_shape=jax.ShapeDtypeStruct((2, 8, 512), jnp.float32),
        in_specs=[vmem] * 3 + [smem] * 3,
        out_specs=vmem,
        scratch_shapes=[
            pltpu.VMEM((2, 512, 512), jnp.bfloat16),
            pltpu.VMEM((4, 128, 512), jnp.bfloat16),
            pltpu.VMEM((2, 4, NX, 8, 512), jnp.float32),
            pltpu.VMEM((4, NX, 2, 4, 8, 512), jnp.bfloat16),
            pltpu.VMEM((4, NX, 2, 4, 8, 512), jnp.bfloat16),
            pltpu.VMEM((4, 2, 4, 8, 512), jnp.float32),
            pltpu.VMEM((4, 4, 2, 8, 512), jnp.bfloat16),
            pltpu.VMEM((NZ, 2, 8, 512), jnp.bfloat16),
            pltpu.VMEM((2, 8, 512), jnp.float32),
            pltpu.SemaphoreType.DMA((4, NX)),
            pltpu.SemaphoreType.DMA((4, NX)),
            pltpu.SemaphoreType.DMA((4, 4)),
            pltpu.SemaphoreType.DMA((NZ,)),
        ],
        compiler_params=pltpu.CompilerParams(collective_id=1, has_side_effects=True),
    )(w, left, right, pairs, targets, live)


def on_device(wave_blocks, left_ops, right_ops, wanted, pairs, targets, live):
    want = jnp.pad(wanted.reshape(NZ, 1, NX * 2), ((0, 0), (0, 0), (0, 128 - NX * 2)))
    w = exchange_wave(wave_blocks, want).reshape(2, 512, 512)
    return sigma_rows(w, left_ops[0], right_ops[0], pairs, targets, live)


def solution(mesh):
    return jax.shard_map(
        on_device,
        mesh=mesh,
        in_specs=(
            P(None, "term", None),
            P("sector", "term", None, None),
            P("sector", "term", None, None),
            P("sector", None, None),
            P("sector", "term", None),
            P("sector", "term", None),
            P("sector", "term"),
        ),
        out_specs=P("sector", "term", None),
        check_vma=False,
    )
```

```python
import jax
import jax.numpy as jnp
from jax import lax
from jax.experimental import pallas as pl
from jax.experimental.pallas import tpu as pltpu
from jax.sharding import PartitionSpec as P

MESH = pl.DeviceIdType.MESH
NX, NY, NZ = 4, 4, 16
SLAB = NX * NY * 2
NZH = NZ // 2
REACH = 4
TILE = 256
GROUP = 4


def place():
    term = lax.axis_index("term")
    sector = lax.axis_index("sector")
    return term // NX, lax.rem(term, NX), sector // 2, lax.rem(sector, 2)


def dev(z, x, y, c):
    return (z * NX + x, y * 2 + c)


def remote(src, dst, send, recv, target):
    return pltpu.make_async_remote_copy(
        src_ref=src, dst_ref=dst, send_sem=send, recv_sem=recv, device_id=target, device_id_type=MESH
    )


def kernel(
    wave_ref, want_ref, l_hbm, r_hbm, pairs, targets, live, out_ref,
    left, right, lp, held1, held2, held3, held4, held5, held6, held7, held8, packed, w_parts, w, want_v, want_s, halves, acc,
    xsend, xrecv, xown, zsend, zrecv, zown,
    load, send1, recv1, send2, recv2, sendw, recvw, sendx, recvx, sendz, recvz,
):
    z, x, y, c = place()
    held = (wave_ref, held1, held2, held3, held4, held5, held6, held7, held8)
    sector = y * 2 + c
    barrier = pltpu.get_barrier_semaphore()

    def along_z(d):
        return lax.rem(z + d + NZ, NZ)

    def slab_core(e):
        return lax.rem(x + e // 8, NX), lax.rem(y + lax.rem(e, 8) // 2, NY), lax.rem(c + e, 2)

    def greet_slab(e, _):
        tx, ty, tc = slab_core(e)
        pl.semaphore_signal(barrier, inc=1, device_id=dev(z, tx, ty, tc), device_id_type=MESH)
        return 0

    for d in range(1, REACH + 1):
        for sign in (1, -1):
            pl.semaphore_signal(barrier, inc=1, device_id=dev(along_z(sign * d), x, y, c), device_id_type=MESH)
    lax.fori_loop(1, SLAB, greet_slab, 0)

    load_left = pltpu.make_async_copy(l_hbm, left, load.at[0])
    load_right = pltpu.make_async_copy(r_hbm, right, load.at[1])
    load_left.start()
    load_right.start()
    pl.semaphore_wait(barrier, 2 * REACH + SLAB - 1)

    cols = pl.ds(pl.multiple_of(y * 128, 128), 128)
    step = jnp.where(c == 0, 1, NZ - 1)

    def direct(i):
        return remote(
            wave_ref.at[:, :, cols], held[i], send1.at[i], recv1.at[i], dev(along_z(step * i), x, y, c)
        )

    def forward(i):
        return remote(
            held[i], held[i + REACH], send1.at[i + REACH], recv1.at[i + REACH],
            dev(along_z(step * REACH), x, y, c),
        )

    def want_copy(e):
        ty, tc = lax.rem(y + e // 2, NY), lax.rem(c + e, 2)
        return remote(want_ref.at[z], want_v.at[sector], sendw.at[e], recvw.at[e], dev(z, x, ty, tc))

    for e in range(1, 8):
        want_copy(e).start()
    for i in range(1, REACH + 1):
        direct(i).start()

    want_v[sector] = want_ref[z]
    for e in range(1, 8):
        want_copy(e).wait()
    want_copy_down = pltpu.make_async_copy(want_v, want_s, load.at[2])
    want_copy_down.start()
    want_copy_down.wait()

    def slab_send(u, from_z, block):
        slot = lax.rem(from_z, NZH)

        def one(e, _):
            tx, ty, tc = slab_core(e)
            for j in range(2):
                packed[u, e - 1, j] = block(want_s[ty * 2 + tc, 0, tx * 2 + j])
            remote(
                packed.at[u, e - 1], w_parts.at[:, c, slot, x, :, cols], send2, recv2, dev(z, tx, ty, tc)
            ).start()
            return 0

        lax.fori_loop(1, SLAB, one, 0)
        for j in range(2):
            w_parts[j, c, slot, x, :, cols] = block(want_s[sector, 0, x * 2 + j])

    @pl.when(c == 1)
    def _():
        slab_send(0, z, lambda source: wave_ref[source, :, cols])

    load_left.wait()
    zb, zm = z // NZH, lax.rem(z, NZH)
    upper = (lax.broadcasted_iota(jnp.int32, (512, 256), 1) // (NX * 8) >= zm) == (zb == 1)
    for a in range(2):
        low, high = left[a, :, :256], left[a, :, 256:]
        lp[a, :, 256:] = jnp.where(upper, high, low)
        lp[a, :, :256] = jnp.where(upper, low, high)

    for i in range(1, NZH + 1):
        direct(i).wait_recv()
        if i <= REACH:
            forward(i).start()
        chunk = held[i]
        if i < NZH:
            slab_send(i - 1 + c, along_z((NZ - step) * i), lambda source: chunk[source])
        else:

            @pl.when(c == 0)
            def _():
                slab_send(i - 1, along_z((NZ - step) * i), lambda source: chunk[source])

    remote(packed, packed, send2, recv2, dev(z, x, y, c)).wait()
    for i in range(1, NZH + 1):
        direct(i).wait_send()

    for j in range(2):
        w[j] = w_parts[j].astype(jnp.float32).reshape(512, 512).astype(jnp.bfloat16)
    for a in range(2):
        for j in range(2):
            for top in range(0, 512, TILE):
                half = jnp.dot(lp[a, top : top + TILE], w[j], preferred_element_type=jnp.float32)
                halves[a * 2 + j, top : top + TILE] = half.astype(jnp.bfloat16)
    load_right.wait()

    def products(h):
        acc[...] = jnp.zeros_like(acc)

        def slots(group, _):
            for top in range(0, 512, TILE):
                total = [None, None]
                for i in range(GROUP):
                    k = group * GROUP + i
                    code = pairs[0, 0, k]
                    product = lax.dot_general(
                        halves[code // 4, top : top + TILE],
                        right[lax.rem(code, 4), h * 256 : (h + 1) * 256],
                        (((1,), (1,)), ((), ())),
                        preferred_element_type=jnp.float32,
                    )
                    used = k < live[0, 0]
                    for t in range(2):
                        part = jnp.where(used & (targets[0, 0, k] == t), product, 0.0)
                        total[t] = part if i == 0 else total[t] + part
                zs = TILE // (NX * 8)
                for t in range(2):
                    acc[t, top // 32 : top // 32 + zs] += total[t].reshape(zs, NX, 8, 256)
            return 0

        lax.fori_loop(0, 12 // GROUP, slots, 0)

    def x_copy(p, e):
        return remote(
            xsend.at[p, e - 1], xrecv.at[p, e - 1], sendx.at[p, e - 1], recvx.at[p, e - 1],
            dev(z, lax.rem(x + e, NX), y, c),
        )

    def start_x(h, t):
        p = h * 2 + t
        for e in range(1, NX):
            xsend[p, e - 1] = acc[t, :, lax.rem(x + e, NX)].astype(jnp.bfloat16)
            x_copy(p, e).start()
        xown[p] = acc[t, :, x]

    def finish_x(h, t):
        p = h * 2 + t
        for e in range(1, NX):
            x_copy(p, e).wait()

        def one(d, _):
            tz = along_z(d)
            total = xown[p, tz]
            for e in range(1, NX):
                total = total + xrecv[p, e - 1, tz].astype(jnp.float32)
            zsend[p, d - 1] = total.astype(jnp.bfloat16)
            remote(zsend.at[p, d - 1], zrecv.at[p, NZ - 1 - d], sendz, recvz, dev(tz, x, y, c)).start()
            return 0

        lax.fori_loop(1, NZ, one, 0)
        total = xown[p, z]
        for e in range(1, NX):
            total = total + xrecv[p, e - 1, z].astype(jnp.float32)
        zown[t, :, h * 256 : (h + 1) * 256] = total

    products(0)
    start_x(0, 0)
    start_x(0, 1)
    products(1)
    start_x(1, 0)
    start_x(1, 1)
    for h in range(2):
        for t in range(2):
            finish_x(h, t)

    remote(zsend, zrecv, sendz, recvz, dev(z, x, y, c)).wait()
    for h in range(2):
        for t in range(2):
            total = zown[t, :, h * 256 : (h + 1) * 256]
            for d in range(NZ - 1):
                total = total + zrecv[h * 2 + t, d].astype(jnp.float32)
            out_ref[t, :, h * 256 : (h + 1) * 256] = total


def on_device(wave_blocks, left_ops, right_ops, wanted, pairs, targets, live):
    want = jnp.pad(wanted.reshape(NZ, 1, NX * 2), ((0, 0), (0, 0), (0, 128 - NX * 2)))
    vmem = pl.BlockSpec(memory_space=pltpu.VMEM)
    smem = pl.BlockSpec(memory_space=pltpu.SMEM)
    hbm = pl.BlockSpec(memory_space=pl.ANY)
    half, full, dma = jnp.bfloat16, jnp.float32, pltpu.SemaphoreType.DMA
    return pl.pallas_call(
        kernel,
        out_shape=jax.ShapeDtypeStruct((2, 8, 512), full),
        in_specs=[vmem, vmem, hbm, hbm, smem, smem, smem],
        out_specs=vmem,
        scratch_shapes=[
            pltpu.VMEM((2, 512, 512), half),
            pltpu.VMEM((4, 512, 512), half),
            pltpu.VMEM((2, 512, 512), half),
            *[pltpu.VMEM((16, 8, 128), half)] * NZH,
            pltpu.VMEM((NZH, SLAB - 1, 2, 8, 128), half),
            pltpu.VMEM((2, 2, NZH, NX, 8, 512), half),
            pltpu.VMEM((2, 512, 512), half),
            pltpu.VMEM((8, 1, 128), jnp.int32),
            pltpu.SMEM((8, 1, 128), jnp.int32),
            pltpu.VMEM((4, 512, 512), half),
            pltpu.VMEM((2, NZ, NX, 8, 256), full),
            pltpu.VMEM((4, NX - 1, NZ, 8, 256), half),
            pltpu.VMEM((4, NX - 1, NZ, 8, 256), half),
            pltpu.VMEM((4, NZ, 8, 256), full),
            pltpu.VMEM((4, NZ - 1, 8, 256), half),
            pltpu.VMEM((4, NZ - 1, 8, 256), half),
            pltpu.VMEM((2, 8, 512), full),
            dma((3,)),
            dma((NZH + 1,)),
            dma((NZH + 1,)),
            dma,
            dma,
            dma((8,)),
            dma((8,)),
            dma((4, NX - 1)),
            dma((4, NX - 1)),
            dma,
            dma,
        ],
        compiler_params=pltpu.CompilerParams(collective_id=0, has_side_effects=True),
    )(wave_blocks, want, left_ops[0], right_ops[0], pairs, targets, live)


def solution(mesh):
    return jax.shard_map(
        on_device,
        mesh=mesh,
        in_specs=(
            P(None, "term", None),
            P("sector", "term", None, None),
            P("sector", "term", None, None),
            P("sector", None, None),
            P("sector", "term", None),
            P("sector", "term", None),
            P("sector", "term"),
        ),
        out_specs=P("sector", "term", None),
        check_vma=False,
    )
```

```python
import jax
import jax.numpy as jnp
from jax import lax
from jax.experimental import pallas as pl
from jax.experimental.pallas import tpu as pltpu
from jax.sharding import PartitionSpec as P

MESH = pl.DeviceIdType.MESH
NX, NY, NZ = 4, 4, 16
NZH = NZ // 2
SLAB = NX * NY * 2
REACH = 3
TAIL = 2
SPREAD = NZH - TAIL
TILE = 256
GROUP = 4


def place():
    term = lax.axis_index("term")
    sector = lax.axis_index("sector")
    return term // NX, lax.rem(term, NX), sector // 2, lax.rem(sector, 2)


def dev(z, x, y, c):
    return (z * NX + x, y * 2 + c)


def remote(src, dst, send, recv, target):
    return pltpu.make_async_remote_copy(
        src_ref=src, dst_ref=dst, send_sem=send, recv_sem=recv, device_id=target, device_id_type=MESH
    )


def kernel(
    wave_ref, want_ref, l_hbm, r_hbm, pairs, targets, live, out_ref,
    left, right, lp, held, rows0, rows1, rows2, rows3, rows4, rows5, packed, late0, late1, late_packed, w_parts, w, want_v, want_s,
    halves, far_acc, near_acc, xsend, xrecv, xown, near_xsend, near_xrecv, near_xown,
    far_send, far_recv, mid_send, mid_recv, near_send, near_recv, zown,
    load, send1, recv1, send2, recv2, send3, recv3, send4, recv4, sendw, recvw, sendx, recvx, sendf, recvf, sendm, recvm,
    sendn, recvn,
):
    z, x, y, c = place()
    zb, zm = z // NZH, lax.rem(z, NZH)
    rows = (rows0, rows1, rows2, rows3, rows4, rows5)
    late = (late0, late1,)
    sector = y * 2 + c
    barrier = pltpu.get_barrier_semaphore()

    def along_z(d):
        return dev(lax.rem(z + d + NZ, NZ), x, y, c)

    def along_x(e):
        return dev(z, lax.rem(x + e, NX), y, c)

    def chip_core(e):
        return lax.rem(y + e // 2, NY), lax.rem(c + e, 2)

    def along_yc(e):
        return dev(z, x, *chip_core(e))

    greeted = [along_z(sign * d) for d in range(1, REACH + 1) for sign in (1, -1)]
    greeted += [along_x(e) for e in range(1, NX)] + [along_yc(e) for e in range(1, 8)]
    for target in greeted:
        pl.semaphore_signal(barrier, inc=1, device_id=target, device_id_type=MESH)
    load_left = pltpu.make_async_copy(l_hbm, left, load.at[0])
    load_right = pltpu.make_async_copy(r_hbm, right, load.at[1])
    load_left.start()
    load_right.start()
    pl.semaphore_wait(barrier, len(greeted))

    cols = pl.ds(pl.multiple_of(y * 128, 128), 128)
    step = jnp.where(c == 0, 1, NZ - 1)

    def direct(i):
        return remote(wave_ref.at[:, :, cols], held.at[i - 1 + c], send1.at[i], recv1.at[i], along_z(step * i))

    def forward(u):
        i = u + 1 - c
        return remote(
            held.at[u], held.at[u + REACH], send1.at[i + REACH], recv1.at[i + REACH], along_z(step * REACH)
        )

    def spread(u, e):
        return remote(held.at[u], rows[u].at[x], send2.at[u, e - 1], recv2.at[u, e - 1], along_x(e))

    def want_copy(e):
        return remote(want_ref.at[0], want_v.at[sector], sendw.at[e], recvw.at[e], along_yc(e))

    for i in range(1, REACH + 1):
        direct(i).start()
    for e in range(1, 8):
        want_copy(e).start()

    def take(u):
        if u == 0:

            @pl.when(c == 1)
            def _():
                held[0] = wave_ref[:, :, cols]

            @pl.when(c == 0)
            def _():
                direct(1).wait_recv()
        else:
            direct(u + 1 - c).wait_recv()
        if u <= NZH - REACH:

            @pl.when((u + 1 - c >= 1) & (u + 1 - c <= NZH - REACH))
            def _():
                forward(u).start()

        if u >= SPREAD:
            late[u - SPREAD][...] = held[u]
            return
        for e in range(1, NX):
            spread(u, e).start()
        rows[u][x] = held[u]

    def select(u):
        for e in range(1, NX):
            spread(u, e).wait_recv()

        def one(e, _):
            ty, tc = chip_core(e)
            for j in range(2):
                packed[u, e - 1, j] = rows[u][:, want_s[ty * 2 + tc, j, z * NX + x]]
            remote(packed.at[u, e - 1], w_parts.at[:, c, u, :, :, cols], send3, recv3, along_yc(e)).start()
            return 0

        lax.fori_loop(1, 8, one, 0)
        for j in range(2):
            w_parts[j, c, u, :, :, cols] = rows[u][:, want_s[sector, j, z * NX + x]]

    def select_late(u):
        chunk, n = late[u - SPREAD], u - SPREAD

        def one(e, _):
            k = lax.rem(e + SLAB // 2 + 4, SLAB)
            tx = lax.rem(x + k // 8, NX)
            ty, tc = chip_core(lax.rem(k, 8))

            @pl.when(k > 0)
            def _():
                for j in range(2):
                    late_packed[n, k - 1, j] = chunk[want_s[ty * 2 + tc, j, z * NX + tx]]
                remote(
                    late_packed.at[n, k - 1], w_parts.at[:, c, u, x, :, cols], send4, recv4, dev(z, tx, ty, tc)
                ).start()

            return 0

        lax.fori_loop(0, SLAB, one, 0)
        for j in range(2):
            w_parts[j, c, u, x, :, cols] = chunk[want_s[sector, j, z * NX + x]]

    take(0)
    want_v[sector] = want_ref[0]

    take(1)
    for e in range(1, 8):
        want_copy(e).wait()
    want_down = pltpu.make_async_copy(want_v, want_s, load.at[2])
    want_down.start()
    take(2)
    want_down.wait()
    select(0)
    for u in range(3, NZH):
        take(u)
        if u >= SPREAD:
            select_late(u)
        if u - 2 < SPREAD:
            select(u - 2)
    for u in range(NZH - 2, SPREAD):
        select(u)

    load_left.wait()
    source = lax.broadcasted_iota(jnp.int32, (512, 512), 0)
    column = lax.broadcasted_iota(jnp.int32, (512, 512), 1)
    u_of = lax.rem(column, 256) // 32
    from_z = jnp.where(column < 256, z + NZ - 1 - u_of, z + u_of)
    wanted_row = lax.rem(from_z, NZ) * 32 + lax.rem(column, 32)
    pick = jnp.where(source == wanted_row, 1.0, 0.0).astype(jnp.bfloat16)
    for a in range(2):
        lp[a] = jnp.dot(left[a], pick, preferred_element_type=jnp.float32).astype(jnp.bfloat16)

    @pl.when(c == 1)
    def _():
        direct(NZH).wait_recv()

    for i in range(1, NZH + 1):
        direct(i).wait_send()
    for u in range(SPREAD):
        for e in range(1, NX):
            spread(u, e).wait_send()
    load_right.wait()
    remote(packed, packed, send3, recv3, along_yc(1)).wait()
    remote(late_packed, late_packed, send4, recv4, along_yc(1)).wait()

    for j in range(2):
        w[j] = w_parts[j].astype(jnp.float32).reshape(512, 512).astype(jnp.bfloat16)

    def half_rows(b):
        return pl.ds(pl.multiple_of(b * TILE, TILE), TILE)

    for a in range(2):
        for j in range(2):
            for top in range(0, 512, TILE):
                half = jnp.dot(lp[a, top : top + TILE], w[j], preferred_element_type=jnp.float32)
                halves[a * 2 + j, top : top + TILE] = half.astype(jnp.bfloat16)

    quarter, zl = z // 4, lax.rem(z, 4)
    sibling = 2 * zb + 1 - lax.rem(quarter, 2)

    def products(p):
        near = p >= 2
        rows_of = pl.ds(pl.multiple_of((sibling if p == 2 else quarter) * 128, 128), 128) if near else half_rows(1 - zb)
        first, last = (0, 512) if near else (p * 256, p * 256 + 256)
        acc = near_acc if near else far_acc
        acc[...] = jnp.zeros_like(acc)

        def slots(group, _):
            total = [None, None]
            for i in range(GROUP):
                k = group * GROUP + i
                code = pairs[0, 0, k]
                product = lax.dot_general(
                    halves[code // 4, rows_of],
                    right[lax.rem(code, 4), first:last],
                    (((1,), (1,)), ((), ())),
                    preferred_element_type=jnp.float32,
                )
                used = k < live[0, 0]
                for t in range(2):
                    part = jnp.where(used & (targets[0, 0, k] == t), product, 0.0)
                    total[t] = part if i == 0 else total[t] + part
            for t in range(2):
                acc[t] += total[t].reshape(acc.shape[1:])
            return 0

        lax.fori_loop(0, 12 // GROUP, slots, 0)

    def x_buffers(p):
        return (near_xsend, near_xrecv, near_xown, near_acc, p - 2) if p >= 2 else (xsend, xrecv, xown, far_acc, p)

    def x_copy(p, e):
        sent, received, _, _, i = x_buffers(p)
        return remote(
            sent.at[i, e - 1], received.at[i, e - 1], sendx.at[p, e - 1], recvx.at[p, e - 1], along_x(e)
        )

    def start_x(p):
        sent, _, own, acc, i = x_buffers(p)
        for e in range(1, NX):
            for t in range(2):
                sent[i, e - 1, t] = acc[t, :, lax.rem(x + e, NX)].astype(jnp.bfloat16)
            x_copy(p, e).start()
        for t in range(2):
            own[i, t] = acc[t, :, x]

    def summed(p, t, zz):
        _, received, own, _, i = x_buffers(p)
        total = own[i, t, zz]
        for e in range(1, NX):
            total = total + received[i, e - 1, t, zz].astype(jnp.float32)
        return total

    def finish_x(p):
        for e in range(1, NX):
            x_copy(p, e).wait()

        def far(zz, _):
            for t in range(2):
                far_send[p, zz, t] = summed(p, t, zz).astype(jnp.bfloat16)
            remote(
                far_send.at[p, zz], far_recv.at[p, zm], sendf, recvf, dev((1 - zb) * NZH + zz, x, y, c)
            ).start()
            return 0

        def next_to(zz, _):
            for t in range(2):
                mid_send[zz, t] = summed(p, t, zz).astype(jnp.bfloat16)
            remote(mid_send.at[zz], mid_recv.at[zl], sendm, recvm, dev(sibling * 4 + zz, x, y, c)).start()
            return 0

        def near(d, _):
            zz = lax.rem(zl + d, 4)
            for t in range(2):
                near_send[d - 1, t] = summed(p, t, zz).astype(jnp.bfloat16)
            remote(
                near_send.at[d - 1], near_recv.at[3 - d], sendn, recvn, dev(quarter * 4 + zz, x, y, c)
            ).start()
            return 0

        if p < 2:
            lax.fori_loop(0, NZH, far, 0)
        elif p == 2:
            lax.fori_loop(0, 4, next_to, 0)
        else:
            lax.fori_loop(1, 4, near, 0)
            for t in range(2):
                zown[t] = summed(p, t, zl)

    for p in range(4):
        products(p)
        start_x(p)
        if p >= 2:
            finish_x(p - 2)
    finish_x(2)
    finish_x(3)

    remote(far_send, far_recv, sendf, recvf, along_yc(1)).wait()
    for h in range(2):
        part = slice(h * 256, h * 256 + 256)
        for t in range(2):
            total = zown[t, :, part]
            for d in range(NZH):
                total = total + far_recv[h, d, t].astype(jnp.float32)
            zown[t, :, part] = total
    remote(mid_send, mid_recv, sendm, recvm, along_yc(1)).wait()
    remote(near_send, near_recv, sendn, recvn, along_yc(1)).wait()
    for t in range(2):
        total = zown[t]
        for d in range(4):
            total = total + mid_recv[d, t].astype(jnp.float32)
        for d in range(3):
            total = total + near_recv[d, t].astype(jnp.float32)
        out_ref[t] = total


def on_device(wave_blocks, left_ops, right_ops, wanted, pairs, targets, live):
    want = jnp.swapaxes(wanted, 1, 2)
    vmem = pl.BlockSpec(memory_space=pltpu.VMEM)
    smem = pl.BlockSpec(memory_space=pltpu.SMEM)
    hbm = pl.BlockSpec(memory_space=pl.ANY)
    half, full, dma = jnp.bfloat16, jnp.float32, pltpu.SemaphoreType.DMA
    return pl.pallas_call(
        kernel,
        out_shape=jax.ShapeDtypeStruct((2, 8, 512), full),
        in_specs=[vmem, vmem, hbm, hbm, smem, smem, smem],
        out_specs=vmem,
        scratch_shapes=[
            pltpu.VMEM((2, 512, 512), half),
            pltpu.VMEM((4, 512, 512), half),
            pltpu.VMEM((2, 512, 512), half),
            pltpu.VMEM((NZH + 1, 16, 8, 128), half),
            *[pltpu.VMEM((NX, 16, 8, 128), half)] * SPREAD,
            pltpu.VMEM((SPREAD, 7, 2, NX, 8, 128), half),
            *[pltpu.VMEM((16, 8, 128), half)] * TAIL,
            pltpu.VMEM((TAIL, SLAB - 1, 2, 8, 128), half),
            pltpu.VMEM((2, 2, NZH, NX, 8, 512), half),
            pltpu.VMEM((2, 512, 512), half),
            pltpu.VMEM((8, 2, 64), jnp.int32),
            pltpu.SMEM((8, 2, 64), jnp.int32),
            pltpu.VMEM((4, 512, 512), half),
            pltpu.VMEM((2, NZH, NX, 8, 256), full),
            pltpu.VMEM((2, 4, NX, 8, 512), full),
            pltpu.VMEM((2, NX - 1, 2, NZH, 8, 256), half),
            pltpu.VMEM((2, NX - 1, 2, NZH, 8, 256), half),
            pltpu.VMEM((2, 2, NZH, 8, 256), full),
            pltpu.VMEM((2, NX - 1, 2, 4, 8, 512), half),
            pltpu.VMEM((2, NX - 1, 2, 4, 8, 512), half),
            pltpu.VMEM((2, 2, 4, 8, 512), full),
            pltpu.VMEM((2, NZH, 2, 8, 256), half),
            pltpu.VMEM((2, NZH, 2, 8, 256), half),
            pltpu.VMEM((4, 2, 8, 512), half),
            pltpu.VMEM((4, 2, 8, 512), half),
            pltpu.VMEM((3, 2, 8, 512), half),
            pltpu.VMEM((3, 2, 8, 512), half),
            pltpu.VMEM((2, 8, 512), full),
            dma((3,)),
            dma((NZH + 1,)),
            dma((NZH + 1,)),
            dma((SPREAD, NX - 1)),
            dma((SPREAD, NX - 1)),
            dma,
            dma,
            dma,
            dma,
            dma((8,)),
            dma((8,)),
            dma((4, NX - 1)),
            dma((4, NX - 1)),
            dma,
            dma,
            dma,
            dma,
            dma,
            dma,
        ],
        compiler_params=pltpu.CompilerParams(collective_id=0, has_side_effects=True),
    )(wave_blocks, want, left_ops[0], right_ops[0], pairs, targets, live)


def solution(mesh):
    return jax.shard_map(
        on_device,
        mesh=mesh,
        in_specs=(
            P(None, "term", None),
            P("sector", "term", None, None),
            P("sector", "term", None, None),
            P("sector", None, None),
            P("sector", "term", None),
            P("sector", "term", None),
            P("sector", "term"),
        ),
        out_specs=P("sector", "term", None),
        check_vma=False,
    )
```

```python
import jax
import jax.numpy as jnp
from jax import lax
from jax.experimental import pallas as pl
from jax.experimental.pallas import tpu as pltpu
from jax.sharding import PartitionSpec as P

MESH = pl.DeviceIdType.MESH
NX, NY, NZ = 4, 4, 16
NZH = NZ // 2
SLAB = NX * NY * 2
REACH = 3
TAIL = 2
SPREAD = NZH - TAIL
TILE = 256
ORDER = (8, 9, 7, 10, 6, 11, 5, 4, -4, 3, -3, 2, 0, 1, -1, -2)
GROUP = 4


def place():
    term = lax.axis_index("term")
    sector = lax.axis_index("sector")
    return term // NX, lax.rem(term, NX), sector // 2, lax.rem(sector, 2)


def dev(z, x, y, c):
    return (z * NX + x, y * 2 + c)


def remote(src, dst, send, recv, target):
    return pltpu.make_async_remote_copy(
        src_ref=src, dst_ref=dst, send_sem=send, recv_sem=recv, device_id=target, device_id_type=MESH
    )


def kernel(
    wave_ref, want_ref, l_hbm, r_hbm, pairs, targets, live, out_ref,
    left, right, lp, held, rows0, rows1, rows2, rows3, rows4, rows5, packed, late0, late1, late_packed, w_parts, w, want_v, want_s,
    halves, far_acc, near_acc, xsend, xrecv, xown, near_xsend, near_xrecv, near_xown,
    far_send, far_recv, mid_send, mid_recv, near_send, near_recv, zown,
    load, send1, recv1, send2, recv2, send3, recv3, send4, recv4, sendw, recvw, sendx, recvx, sendf, recvf, sendm, recvm,
    sendn, recvn,
):
    z, x, y, c = place()
    rows = (rows0, rows1, rows2, rows3, rows4, rows5)
    late = (late0, late1,)
    sector = y * 2 + c
    barrier = pltpu.get_barrier_semaphore()

    def along_z(d):
        return dev(lax.rem(z + d + NZ, NZ), x, y, c)

    def along_x(e):
        return dev(z, lax.rem(x + e, NX), y, c)

    def chip_core(e):
        return lax.rem(y + e // 2, NY), lax.rem(c + e, 2)

    def along_yc(e):
        return dev(z, x, *chip_core(e))

    greeted = [along_z(sign * d) for d in range(1, REACH + 1) for sign in (1, -1)]
    greeted += [along_x(e) for e in range(1, NX)] + [along_yc(e) for e in range(1, 8)]
    for target in greeted:
        pl.semaphore_signal(barrier, inc=1, device_id=target, device_id_type=MESH)
    load_right = pltpu.make_async_copy(r_hbm, right, load.at[1])
    for k, d in enumerate(ORDER):
        taken = pl.ds(pl.multiple_of(lax.rem(z + d + NZ, NZ) * 32, 32), 32)
        pltpu.make_async_copy(l_hbm.at[:, taken, :], left.at[:, k * 32 : k * 32 + 32, :], load.at[0]).start()
    load_right.start()
    pl.semaphore_wait(barrier, len(greeted))

    cols = pl.ds(pl.multiple_of(y * 128, 128), 128)
    step = jnp.where(c == 0, 1, NZ - 1)

    def direct(i):
        return remote(wave_ref.at[:, :, cols], held.at[i - 1 + c], send1.at[i], recv1.at[i], along_z(step * i))

    def forward(u):
        i = u + 1 - c
        return remote(
            held.at[u], held.at[u + REACH], send1.at[i + REACH], recv1.at[i + REACH], along_z(step * REACH)
        )

    def spread(u, e):
        return remote(held.at[u], rows[u].at[x], send2.at[u, e - 1], recv2.at[u, e - 1], along_x(e))

    def want_copy(e):
        return remote(want_ref.at[0], want_v.at[sector], sendw.at[e], recvw.at[e], along_yc(e))

    for i in range(1, REACH + 1):
        direct(i).start()
    for e in range(1, 8):
        want_copy(e).start()

    def take(u):
        if u == 0:

            @pl.when(c == 1)
            def _():
                held[0] = wave_ref[:, :, cols]

            @pl.when(c == 0)
            def _():
                direct(1).wait_recv()
        else:
            direct(u + 1 - c).wait_recv()
        if u <= NZH - REACH:

            @pl.when((u + 1 - c >= 1) & (u + 1 - c <= NZH - REACH))
            def _():
                forward(u).start()

        if u >= SPREAD:
            late[u - SPREAD][...] = held[u]
            return
        for e in range(1, NX):
            spread(u, e).start()
        rows[u][x] = held[u]

    def select(u):
        for e in range(1, NX):
            spread(u, e).wait_recv()

        def one(e, _):
            ty, tc = chip_core(e)
            for j in range(2):
                packed[u, e - 1, j] = rows[u][:, want_s[ty * 2 + tc, j, z * NX + x]]
            remote(packed.at[u, e - 1], w_parts.at[:, c, u, :, :, cols], send3, recv3, along_yc(e)).start()
            return 0

        lax.fori_loop(1, 8, one, 0)
        for j in range(2):
            w_parts[j, c, u, :, :, cols] = rows[u][:, want_s[sector, j, z * NX + x]]

    def select_late(u):
        chunk, n = late[u - SPREAD], u - SPREAD

        def one(e, _):
            k = lax.rem(e + SLAB // 2 + 4, SLAB)
            tx = lax.rem(x + k // 8, NX)
            ty, tc = chip_core(lax.rem(k, 8))

            @pl.when(k > 0)
            def _():
                for j in range(2):
                    late_packed[n, k - 1, j] = chunk[want_s[ty * 2 + tc, j, z * NX + tx]]
                remote(
                    late_packed.at[n, k - 1], w_parts.at[:, c, u, x, :, cols], send4, recv4, dev(z, tx, ty, tc)
                ).start()

            return 0

        lax.fori_loop(0, SLAB, one, 0)
        for j in range(2):
            w_parts[j, c, u, x, :, cols] = chunk[want_s[sector, j, z * NX + x]]

    take(0)
    want_v[sector] = want_ref[0]

    take(1)
    for e in range(1, 8):
        want_copy(e).wait()
    want_down = pltpu.make_async_copy(want_v, want_s, load.at[2])
    want_down.start()
    take(2)
    want_down.wait()
    select(0)
    for u in range(3, NZH):
        take(u)
        if u >= SPREAD:
            select_late(u)
        if u - 2 < SPREAD:
            select(u - 2)
    for u in range(NZH - 2, SPREAD):
        select(u)

    pltpu.make_async_copy(l_hbm, left, load.at[0]).wait()
    source = lax.broadcasted_iota(jnp.int32, (512, 512), 0)
    column = lax.broadcasted_iota(jnp.int32, (512, 512), 1)
    u_of = lax.rem(column, 256) // 32
    from_z = jnp.where(column < 256, z + NZ - 1 - u_of, z + u_of)
    wanted_row = lax.rem(from_z, NZ) * 32 + lax.rem(column, 32)
    pick = jnp.where(source == wanted_row, 1.0, 0.0).astype(jnp.bfloat16)
    for a in range(2):
        lp[a] = jnp.dot(left[a], pick, preferred_element_type=jnp.float32).astype(jnp.bfloat16)

    @pl.when(c == 1)
    def _():
        direct(NZH).wait_recv()

    for i in range(1, NZH + 1):
        direct(i).wait_send()
    for u in range(SPREAD):
        for e in range(1, NX):
            spread(u, e).wait_send()
    load_right.wait()
    remote(packed, packed, send3, recv3, along_yc(1)).wait()
    remote(late_packed, late_packed, send4, recv4, along_yc(1)).wait()

    for j in range(2):
        w[j] = w_parts[j].astype(jnp.float32).reshape(512, 512).astype(jnp.bfloat16)

    for a in range(2):
        for j in range(2):
            for top in range(0, 512, TILE):
                half = jnp.dot(lp[a, top : top + TILE], w[j], preferred_element_type=jnp.float32)
                halves[a * 2 + j, top : top + TILE] = half.astype(jnp.bfloat16)

    def products(p):
        near = p >= 2
        top, bottom = (p * 128, p * 128 + 128) if near else (0, 256)
        first, last = (0, 512) if near else (p * 256, p * 256 + 256)
        acc = near_acc if near else far_acc
        acc[...] = jnp.zeros_like(acc)

        def slots(group, _):
            total = [None, None]
            for i in range(GROUP):
                k = group * GROUP + i
                code = pairs[0, 0, k]
                product = lax.dot_general(
                    halves[code // 4, top:bottom],
                    right[lax.rem(code, 4), first:last],
                    (((1,), (1,)), ((), ())),
                    preferred_element_type=jnp.float32,
                )
                used = k < live[0, 0]
                for t in range(2):
                    part = jnp.where(used & (targets[0, 0, k] == t), product, 0.0)
                    total[t] = part if i == 0 else total[t] + part
            for t in range(2):
                acc[t] += total[t].reshape(acc.shape[1:])
            return 0

        lax.fori_loop(0, 12 // GROUP, slots, 0)

    def x_buffers(p):
        return (near_xsend, near_xrecv, near_xown, near_acc, p - 2) if p >= 2 else (xsend, xrecv, xown, far_acc, p)

    def x_copy(p, t, e):
        sent, received, _, _, i = x_buffers(p)
        return remote(
            sent.at[i, e - 1, t], received.at[i, e - 1, t], sendx.at[p, t, e - 1], recvx.at[p, t, e - 1], along_x(e)
        )

    def start_x(p):
        sent, _, own, acc, i = x_buffers(p)
        for t in range(2):
            for e in range(1, NX):
                sent[i, e - 1, t] = acc[t, :, lax.rem(x + e, NX)].astype(jnp.bfloat16)
                x_copy(p, t, e).start()
            own[i, t] = acc[t, :, x]

    def finish_x(p, t):
        _, received, own, _, i = x_buffers(p)
        for e in range(1, NX):
            x_copy(p, t, e).wait()
        for k in range(NZH if p < 2 else 4):
            total = own[i, t, k]
            for e in range(1, NX):
                total = total + received[i, e - 1, t, k].astype(jnp.float32)
            d = ORDER[k if p < 2 else p * 4 + k]
            if d == 0:
                zown[t] = total
                continue
            if p < 2:
                sent, landed, send, recv = far_send.at[p, k, t], far_recv.at[p, k, t], sendf, recvf
            elif p == 2:
                sent, landed, send, recv = mid_send.at[k, t], mid_recv.at[k, t], sendm, recvm
            else:
                sent, landed, send, recv = near_send.at[k - 1, t], near_recv.at[k - 1, t], sendn, recvn
            sent[...] = total.astype(jnp.bfloat16)
            remote(sent, landed, send, recv, along_z(d)).start()

    for p in range(4):
        products(p)
        start_x(p)
        if p >= 1:
            finish_x(p - 1, 0)
            finish_x(p - 1, 1)
    finish_x(3, 0)
    finish_x(3, 1)

    remote(far_send, far_recv, sendf, recvf, along_yc(1)).wait()
    for h in range(2):
        part = slice(h * 256, h * 256 + 256)
        for t in range(2):
            total = zown[t, :, part]
            for d in range(NZH):
                total = total + far_recv[h, d, t].astype(jnp.float32)
            zown[t, :, part] = total
    remote(mid_send, mid_recv, sendm, recvm, along_yc(1)).wait()
    remote(near_send, near_recv, sendn, recvn, along_yc(1)).wait()
    for t in range(2):
        total = zown[t]
        for d in range(4):
            total = total + mid_recv[d, t].astype(jnp.float32)
        for d in range(3):
            total = total + near_recv[d, t].astype(jnp.float32)
        out_ref[t] = total


def on_device(wave_blocks, left_ops, right_ops, wanted, pairs, targets, live):
    want = jnp.swapaxes(wanted, 1, 2)
    vmem = pl.BlockSpec(memory_space=pltpu.VMEM)
    smem = pl.BlockSpec(memory_space=pltpu.SMEM)
    hbm = pl.BlockSpec(memory_space=pl.ANY)
    half, full, dma = jnp.bfloat16, jnp.float32, pltpu.SemaphoreType.DMA
    return pl.pallas_call(
        kernel,
        out_shape=jax.ShapeDtypeStruct((2, 8, 512), full),
        in_specs=[vmem, vmem, hbm, hbm, smem, smem, smem],
        out_specs=vmem,
        scratch_shapes=[
            pltpu.VMEM((2, 512, 512), half),
            pltpu.VMEM((4, 512, 512), half),
            pltpu.VMEM((2, 512, 512), half),
            pltpu.VMEM((NZH + 1, 16, 8, 128), half),
            *[pltpu.VMEM((NX, 16, 8, 128), half)] * SPREAD,
            pltpu.VMEM((SPREAD, 7, 2, NX, 8, 128), half),
            *[pltpu.VMEM((16, 8, 128), half)] * TAIL,
            pltpu.VMEM((TAIL, SLAB - 1, 2, 8, 128), half),
            pltpu.VMEM((2, 2, NZH, NX, 8, 512), half),
            pltpu.VMEM((2, 512, 512), half),
            pltpu.VMEM((8, 2, 64), jnp.int32),
            pltpu.SMEM((8, 2, 64), jnp.int32),
            pltpu.VMEM((4, 512, 512), half),
            pltpu.VMEM((2, NZH, NX, 8, 256), full),
            pltpu.VMEM((2, 4, NX, 8, 512), full),
            pltpu.VMEM((2, NX - 1, 2, NZH, 8, 256), half),
            pltpu.VMEM((2, NX - 1, 2, NZH, 8, 256), half),
            pltpu.VMEM((2, 2, NZH, 8, 256), full),
            pltpu.VMEM((2, NX - 1, 2, 4, 8, 512), half),
            pltpu.VMEM((2, NX - 1, 2, 4, 8, 512), half),
            pltpu.VMEM((2, 2, 4, 8, 512), full),
            pltpu.VMEM((2, NZH, 2, 8, 256), half),
            pltpu.VMEM((2, NZH, 2, 8, 256), half),
            pltpu.VMEM((4, 2, 8, 512), half),
            pltpu.VMEM((4, 2, 8, 512), half),
            pltpu.VMEM((3, 2, 8, 512), half),
            pltpu.VMEM((3, 2, 8, 512), half),
            pltpu.VMEM((2, 8, 512), full),
            dma((3,)),
            dma((NZH + 1,)),
            dma((NZH + 1,)),
            dma((SPREAD, NX - 1)),
            dma((SPREAD, NX - 1)),
            dma,
            dma,
            dma,
            dma,
            dma((8,)),
            dma((8,)),
            dma((4, 2, NX - 1)),
            dma((4, 2, NX - 1)),
            dma,
            dma,
            dma,
            dma,
            dma,
            dma,
        ],
        compiler_params=pltpu.CompilerParams(collective_id=0, has_side_effects=True),
    )(wave_blocks, want, left_ops[0], right_ops[0], pairs, targets, live)


def solution(mesh):
    return jax.shard_map(
        on_device,
        mesh=mesh,
        in_specs=(
            P(None, "term", None),
            P("sector", "term", None, None),
            P("sector", "term", None, None),
            P("sector", None, None),
            P("sector", "term", None),
            P("sector", "term", None),
            P("sector", "term"),
        ),
        out_specs=P("sector", "term", None),
        check_vma=False,
    )
```
